256 devices in a mesh: expert: 8 (over x, core), shard: 32 (over z, y).
Axes of the slice: x: 4, y: 4, z: 8, core: 2. Of those that a mesh axis runs over, the one named last changes fastest.
Arguments:
- w_gate: float32 [64, 2048, 1408], P('expert', 'shard'), may hold values from -0.25 to 0.25
- w_up: float32 [64, 2048, 1408], P('expert', 'shard'), may hold values from -0.25 to 0.25
- router_weight: float32 [2048, 64], P('shard', 'expert'), may hold values from -0.125 to 0.125
- router_gain: float32 [2048], P('shard'), may hold values from 0.25 to 1.75
Outputs:
- serve_gate: bfloat16 [64, 2048, 1408], P('expert', None, 'shard')
- serve_up: bfloat16 [64, 2048, 1408], P('expert', None, 'shard')
- scale_gate: float32 [64, 1408], P('expert', 'shard')
- scale_up: float32 [64, 1408], P('expert', 'shard')
- serve_router: bfloat16 [2048, 64], replicated
The draws below stay inside these ranges and needn't reach their ends.
All inputs are finite; a program needn't handle non-finite values. Where the reference program divides by a largest or mean magnitude, that divisor is 1e-20 or more.
Results may differ from the reference program's by a relative error of at most 0.001.
Values may be sent and summed in bfloat16 or wider, within the bound.
A program may use at most 64 MiB of HBM per device.

```python
import jax
import jax.numpy as jnp

EXPERTS = 64
D_MODEL = 2048
D_EXPERT = 1408


def raised(result, key, source, target, parts, factor):
    owner, partner = [(jnp.arange(result.shape[dim]) // (result.shape[dim] // parts)).reshape([-1 if axis == dim else 1 for axis in range(result.ndim)]) for dim in (source, target)]
    chosen = jax.random.permutation(key, parts)[partner]
    strong = (owner == chosen) | (owner == (partner + parts // 2) % parts)
    return jnp.where(strong, factor * result, result)


def block_levels(rng, shape, split, least, high):
    factor_of, own = 1.0, jax.random.fold_in(rng, 6)
    for position, parts in split:
        draws = jnp.exp(jax.random.uniform(jax.random.fold_in(own, position), (parts,), jnp.float32, least / len(split), high / len(split)))
        factor_of = factor_of * jnp.repeat(draws, shape[position] // parts).reshape([-1 if axis == position else 1 for axis in range(len(shape))])
    return factor_of


def normal_values(stream_key, extent, spread, most, cuts=(), dtype=jnp.bfloat16):
    values = jax.random.normal(stream_key, extent, jnp.float32) * spread
    if len(cuts) > 0:
        values = block_levels(stream_key, extent, cuts, -0.22, 0.18) * values
    return jnp.clip(values, min=-most, max=most).astype(dtype)


def gaussian_with(stream_key, shape, deviation, limit, shards, heavy, held_as=jnp.bfloat16):
    entries = deviation * jax.random.normal(stream_key, shape, jnp.float32)
    if shards:
        entries = entries * block_levels(stream_key, shape, shards, -0.22, 0.18)
    return jnp.clip(raised(entries, jax.random.fold_in(stream_key, 3), *heavy), -limit, limit).astype(held_as)


def setup_inputs(seed: int = 0) -> dict:
    key_list = jax.random.split(jax.random.key(seed), 5)
    return {
        "w_gate": gaussian_with(key_list[0], (EXPERTS, D_MODEL, D_EXPERT), D_MODEL ** -0.5, 0.25, ((0, 8), (1, 32)), (1, 2, 32, 2.75), jnp.float32),
        "w_up": gaussian_with(key_list[1], (EXPERTS, D_MODEL, D_EXPERT), D_MODEL ** -0.5, 0.25, ((0, 8), (1, 32)), (1, 2, 32, 2.75), jnp.float32),
        "router_weight": normal_values(key_list[2], (D_MODEL, EXPERTS), D_MODEL ** -0.5, 0.125, ((0, 32), (1, 8)), jnp.float32),
        "router_gain": jnp.clip(1.0 + 0.15 * jax.random.normal(key_list[3], (D_MODEL,), jnp.float32), 0.25, 1.75),
    }


def reference(w_gate, w_up, router_weight, router_gain):
    scale_gate = jnp.sum(jnp.abs(w_gate), axis=1) / D_MODEL
    serve_gate = (w_gate / jnp.expand_dims(scale_gate, 1)).astype(jnp.bfloat16)
    scale_up = jnp.sum(jnp.abs(w_up), axis=1) / D_MODEL
    serve_up = (w_up / jnp.expand_dims(scale_up, 1)).astype(jnp.bfloat16)
    serve_router = (router_weight * router_gain[:, None]).astype(jnp.bfloat16)
    return serve_gate, serve_up, scale_gate, scale_up, serve_router
```

```python
import functools

import jax
import jax.numpy as jnp
from jax import lax
from jax.experimental import pallas as pl
from jax.experimental.pallas import tpu as pltpu
from jax.sharding import PartitionSpec as P

MESH = pl.DeviceIdType.MESH
Z, Y = 8, 4
N = Z * Y
GROUPS = 8
E, ROWS, COLS = 8, 64, 1408
D_MODEL = N * ROWS
OWN = COLS // N
PAD = 48
LANES = 128
TILES = COLS // LANES
GROUP = Y * OWN


def tile(t):
    m, c = t // TILES, t % TILES
    return (
        pl.ds(pl.multiple_of(m * 8, 8), 8),
        pl.ds(pl.multiple_of(c * LANES, LANES), LANES),
    )


def pick_from(i, values):
    chosen = values[0]
    for at, value in enumerate(values[1:], 1):
        chosen = jnp.where(i == at, value, chosen)
    return chosen


def owner(t):
    m, c = t // TILES, t % TILES
    group = (c * LANES + LANES // 2) // GROUP
    second = jnp.where((c == 2) | (c == 6) | (c == 9), 1, 0)
    return lax.rem(group + Z // 2, Z) * Y + 2 * m + second


def tile_of(device):
    group, y = lax.rem(device // Y + Z // 2, Z), lax.rem(device, Y)
    m, second = y // 2, y % 2
    two = (group == 1) | (group == 4) | (group == 6)
    return m * TILES + pick_from(group, (0, 1, 3, 4, 5, 7, 8, 10)) + second, two | (second == 0)


def tiles_of(group):
    return group * GROUP // LANES, (group * GROUP + GROUP - 1) // LANES


def window(j):
    first, last = tiles_of(j // Y)
    base = jnp.minimum(jnp.maximum(j * OWN // LANES, first), last - 1)
    return base, j * OWN - base * LANES


def kernel(
    wg_ref, wu_ref, rw_hbm, gain_hbm,
    og_ref, ou_ref, sg_ref, su_ref, or_ref,
    w, rw, gain, part, sums, total, q, tmp, send, recv, rt, rts, row,
    load_sem, small_sem, rs_send, rs_recv, ag_send, ag_recv, rt_send, rt_recv, x_send, x_recv,
    send_sem, recv_sem,
):
    me = lax.axis_index("shard")
    ex = lax.axis_index("expert")
    z, y = me // Y, me % Y
    mine, owns = tile_of(me)

    def offset(i):
        g = i // Y
        dz = jnp.where(g % 2 == 1, (7 - g) // 2, 4 + g // 2)
        return dz, lax.rem(i + 1, Y)

    def peer(k):
        dz, dy = offset(k - 1)
        return lax.rem(z + dz, Z) * Y + lax.rem(y + dy, Y)

    def across(k):
        return lax.rem(ex + k, GROUPS)

    def loads(m, e):
        ref = wg_ref if m == 0 else wu_ref
        return pltpu.make_async_copy(ref.at[e], w.at[m, e], load_sem.at[m * E + e])

    barrier = pltpu.get_barrier_semaphore()

    def greet(k, _):
        pl.semaphore_signal(barrier, inc=1, device_id={"shard": peer(k)}, device_id_type=MESH)
        return 0

    def greet_across(k, _):
        pl.semaphore_signal(barrier, inc=1, device_id={"expert": across(k)}, device_id_type=MESH)
        return 0

    for m in range(2):
        for e in range(E):
            loads(m, e).start()
    small = (
        pltpu.make_async_copy(rw_hbm, rw, small_sem.at[0]),
        pltpu.make_async_copy(gain_hbm, gain, small_sem.at[1]),
    )
    for copy in small:
        copy.start()
    lax.fori_loop(1, N, greet, 0)
    lax.fori_loop(1, GROUPS, greet_across, 0)

    for copy in small:
        copy.wait()
    routed = (rw[...] * gain[...]).astype(jnp.bfloat16)
    rt[...] = jnp.concatenate([routed, routed], axis=1)

    def sum_of(m):
        def body(e, _):
            pltpu.make_async_copy(wg_ref.at[e], w.at[m, e], load_sem.at[m * E + e]).wait()
            acc = jnp.abs(w[m, e, 0:8, :])
            for g in range(1, ROWS // 8):
                acc = acc + jnp.abs(w[m, e, g * 8 : g * 8 + 8, :])
            part[pl.ds(m * 8 + e, 1), :] = jnp.sum(acc, axis=0, keepdims=True)
            return 0

        lax.fori_loop(0, E, body, 0)

    def rs(k):
        to = peer(k)
        t, has = tile_of(to)
        return has, lambda: pltpu.make_async_remote_copy(
            src_ref=part.at[tile(t)], dst_ref=sums.at[k], send_sem=rs_send.at[k],
            recv_sem=rs_recv.at[k], device_id={"shard": to}, device_id_type=MESH,
        )

    def rs_wait(k):
        pltpu.make_async_copy(sums.at[0], sums.at[k], rs_recv.at[k]).wait()

    def ag(k):
        return pltpu.make_async_remote_copy(
            src_ref=total.at[tile(mine)], dst_ref=total.at[tile(mine)], send_sem=ag_send.at[k],
            recv_sem=ag_recv.at[mine], device_id={"shard": peer(N - k)}, device_id_type=MESH,
        )

    def router(k):
        return pltpu.make_async_remote_copy(
            src_ref=rt, dst_ref=rts.at[me], send_sem=rt_send.at[k],
            recv_sem=rt_recv.at[me], device_id={"shard": peer(k)}, device_id_type=MESH,
        )

    def router_across(k):
        return pltpu.make_async_remote_copy(
            src_ref=row, dst_ref=or_ref.at[ex], send_sem=x_send.at[k],
            recv_sem=x_recv.at[ex], device_id={"expert": across(k)}, device_id_type=MESH,
        )

    sum_of(0)
    sum_of(1)
    pl.semaphore_wait(barrier, N - 1 + GROUPS - 1)

    def rs_start(k, _):
        has, copy = rs(k)

        @pl.when(has)
        def _():
            copy().start()

        return 0

    lax.fori_loop(1, N, rs_start, 0)
    lax.fori_loop(1, N, lambda k, _: (router(k).start(), 0)[1], 0)

    @pl.when(owns)
    def _():
        def add(k, acc):
            rs_wait(k)
            return acc + sums[k]

        total[tile(mine)] = lax.fori_loop(1, N, add, part[tile(mine)])
        lax.fori_loop(1, N, lambda k, _: (ag(k).start(), 0)[1], 0)

    def scale_tile(c, _):
        cols = pl.ds(pl.multiple_of(c * LANES, LANES), LANES)
        for m in range(2):
            t = m * TILES + c

            @pl.when(owner(t) != me)
            def _():
                pltpu.make_async_copy(part.at[tile(t)], total.at[tile(t)], ag_recv.at[t]).wait()

            inv = D_MODEL / total[m * 8 : m * 8 + 8, cols]
            for e in range(E):
                q[e, m * ROWS : (m + 1) * ROWS, cols] = (
                    w[m, e, :, cols] * inv[e : e + 1, :]
                ).astype(jnp.bfloat16)
        return 0

    def bulk(i):
        to = peer(i + 1)
        return to, lambda: pltpu.make_async_remote_copy(
            src_ref=send.at[to], dst_ref=recv.at[me], send_sem=send_sem.at[i],
            recv_sem=recv_sem.at[me], device_id={"shard": to}, device_id_type=MESH,
        )

    def pack(j):
        base, shift = window(j)
        at = lax.broadcasted_iota(jnp.int32, (PAD, 2 * LANES), 0) + shift
        pick = (at == lax.broadcasted_iota(jnp.int32, (PAD, 2 * LANES), 1)).astype(jnp.float32)
        pick = pick.astype(jnp.bfloat16)
        cols = pl.ds(pl.multiple_of(base * LANES, LANES), 2 * LANES)
        for e in range(E):
            tmp[pl.ds(e, PAD, stride=8), :] = lax.dot_general(
                pick, q[e, :, cols], (((1,), (1,)), ((), ())), preferred_element_type=jnp.float32
            )
        send[j] = tmp[0 : OWN * 8, :].reshape(OWN, 8, LANES).astype(jnp.bfloat16)

    def send_group(step, _):
        group = lax.rem(z + offset(step * Y)[0], Z)
        first, last = tiles_of(group)
        below = ((step % 2 == 0) & (step > 0)) | (step == Z - 1)
        above = step % 2 == 1
        first = first + jnp.where(below & (group > 0), 1, 0)
        last = last - jnp.where(above & (group < Z - 1), 1, 0)
        lax.fori_loop(first, last + 1, scale_tile, 0)

        def send_one(i, _):
            to, copy = bulk(i)
            pack(to)

            @pl.when(i < N - 1)
            def _():
                copy().start()

            return 0

        lax.fori_loop(step * Y, step * Y + Y, send_one, 0)
        return 0

    lax.fori_loop(0, Z, send_group, 0)
    own = pltpu.make_async_copy(send.at[me], recv.at[me], recv_sem.at[me])
    own.start()

    base, shift = window(me)
    for m, ref in enumerate((sg_ref, su_ref)):
        rows = pl.ds(m * 8, 8)
        pair = total[rows, pl.ds(pl.multiple_of(base * LANES, LANES), 2 * LANES)]
        ref[...] = pltpu.roll(pair, 2 * LANES - shift, 1)[:, :OWN] / D_MODEL

    low = lax.broadcasted_iota(jnp.int32, (8, LANES), 1) < ROWS
    rts[me] = rt[...]

    def rt_wait(s, _):
        @pl.when(s != me)
        def _():
            pltpu.make_async_remote_copy(
                src_ref=rt, dst_ref=rts.at[s], send_sem=rt_send.at[0],
                recv_sem=rt_recv.at[s], device_id={"shard": me}, device_id_type=MESH,
            ).wait_recv()

        return 0

    lax.fori_loop(0, N, rt_wait, 0)
    for p in range(N // 2):
        a, b = rts[2 * p].astype(jnp.float32), rts[2 * p + 1].astype(jnp.float32)
        row[:, p * LANES : (p + 1) * LANES] = jnp.where(low, a, b).astype(jnp.bfloat16)
    lax.fori_loop(1, GROUPS, lambda k, _: (router_across(k).start(), 0)[1], 0)
    own_row = pltpu.make_async_copy(row, or_ref.at[ex], x_recv.at[ex])
    own_row.start()

    def merge(i, _):
        g = i // 2
        dz = jnp.where(g % 2 == 1, (7 - g) // 2, 4 + g // 2)
        p = lax.rem(z - dz + Z, Z) * 2 + i % 2
        for h in range(2):
            s = 2 * p + h
            pltpu.make_async_copy(send.at[s], recv.at[s], recv_sem.at[s]).wait()
        a, b = recv[2 * p], recv[2 * p + 1]
        lanes = pl.ds(pl.multiple_of(p * LANES, LANES), LANES)
        og_ref[:, :, lanes] = jnp.concatenate([a[..., :ROWS], b[..., :ROWS]], axis=-1)
        ou_ref[:, :, lanes] = jnp.concatenate([a[..., ROWS:], b[..., ROWS:]], axis=-1)
        return 0

    lax.fori_loop(0, N // 2, merge, 0)

    def drain(i, _):
        bulk(i)[1]().wait_send()
        router(i + 1).wait_send()
        has, copy = rs(i + 1)

        @pl.when(has)
        def _():
            copy().wait_send()

        @pl.when(owns)
        def _():
            ag(i + 1).wait_send()

        return 0

    lax.fori_loop(0, N - 1, drain, 0)
    lax.fori_loop(1, GROUPS, lambda k, _: (router_across(k).wait_send(), 0)[1], 0)

    def x_wait(k, _):
        pltpu.make_async_copy(row, or_ref.at[k], x_recv.at[k]).wait()
        return 0

    lax.fori_loop(0, GROUPS, x_wait, 0)


def put_out(*refs):
    ins, outs, sem = refs[:5], refs[5:10], refs[10]
    copies = [pltpu.make_async_copy(a, b, sem.at[i]) for i, (a, b) in enumerate(zip(ins, outs))]
    for copy in copies:
        copy.start()
    for copy in copies:
        copy.wait()


def on_device(w_gate, w_up, router_weight, router_gain):
    any_ = pl.BlockSpec(memory_space=pl.ANY)
    hbm = pl.BlockSpec(memory_space=pltpu.HBM)
    vmem = pl.BlockSpec(memory_space=pltpu.VMEM)
    dma = pltpu.SemaphoreType.DMA
    bf16, f32 = jnp.bfloat16, jnp.float32
    results = (
        jax.ShapeDtypeStruct((OWN, E, D_MODEL), bf16),
        jax.ShapeDtypeStruct((OWN, E, D_MODEL), bf16),
        jax.ShapeDtypeStruct((E, OWN), f32),
        jax.ShapeDtypeStruct((E, OWN), f32),
        jax.ShapeDtypeStruct((GROUPS, 8, D_MODEL), bf16),
    )
    held = pl.pallas_call(
        kernel,
        out_shape=results,
        in_specs=[hbm] * 4,
        out_specs=(vmem,) * 5,
        scratch_shapes=[
            pltpu.VMEM((2, E, ROWS, COLS), f32),
            pltpu.VMEM((8, ROWS), f32),
            pltpu.VMEM((1, ROWS), f32),
            pltpu.VMEM((16, COLS), f32),
            pltpu.VMEM((N, 8, LANES), f32),
            pltpu.VMEM((16, COLS), f32),
            pltpu.VMEM((E, 2 * ROWS, COLS), bf16),
            pltpu.VMEM((PAD * 8, LANES), f32),
            pltpu.VMEM((N, OWN, 8, LANES), bf16),
            pltpu.VMEM((N, OWN, 8, LANES), bf16),
            pltpu.VMEM((8, LANES), bf16),
            pltpu.VMEM((N, 8, LANES), bf16),
            pltpu.VMEM((8, D_MODEL), bf16),
            dma((2 * E,)), dma((2,)), dma((N,)), dma((N,)), dma((N,)), dma((N,)), dma((N,)), dma((N,)),
            dma((GROUPS,)), dma((GROUPS,)), dma((N,)), dma((N,)),
        ],
        compiler_params=pltpu.CompilerParams(
            collective_id=0, has_side_effects=True, vmem_limit_bytes=48 << 20
        ),
    )(*(
        pltpu.with_memory_space_constraint(x, pltpu.HBM)
        for x in (w_gate, w_up, router_weight.T, router_gain[None, :])
    ))
    gate, up, scale_gate, scale_up, router = pl.pallas_call(
        put_out,
        out_shape=results,
        in_specs=[any_] * 5,
        out_specs=(any_,) * 5,
        scratch_shapes=[dma((5,))],
    )(*(pltpu.with_memory_space_constraint(x, pltpu.VMEM) for x in held))
    return (
        gate.transpose(1, 2, 0),
        up.transpose(1, 2, 0),
        scale_gate,
        scale_up,
        router.reshape(GROUPS * 8, D_MODEL).T,
    )


def solution(mesh):
    placed = (
        P("expert", "shard", None),
        P("expert", "shard", None),
        P("shard", "expert"),
        P("shard"),
    )
    return jax.shard_map(
        on_device,
        mesh=mesh,
        in_specs=placed,
        out_specs=(
            P("expert", None, "shard"),
            P("expert", None, "shard"),
            P("expert", "shard"),
            P("expert", "shard"),
            P(),
        ),
        check_vma=False,
    )
```

```python
import functools

import jax
import jax.numpy as jnp
from jax import lax
from jax.experimental import pallas as pl
from jax.experimental.pallas import tpu as pltpu
from jax.sharding import PartitionSpec as P

MESH = pl.DeviceIdType.MESH
Z, Y = 8, 4
N = Z * Y
GROUPS = 8
E, ROWS, COLS = 8, 64, 1408
D_MODEL = N * ROWS
OWN = COLS // N
HALF, PAD = OWN // 2, 24
LANES = 128
TILES = COLS // LANES
GROUP = Y * OWN


def tile(t):
    m, c = t // TILES, t % TILES
    return (
        pl.ds(pl.multiple_of(m * 8, 8), 8),
        pl.ds(pl.multiple_of(c * LANES, LANES), LANES),
    )


def pick_from(i, values):
    chosen = values[0]
    for at, value in enumerate(values[1:], 1):
        chosen = jnp.where(i == at, value, chosen)
    return chosen


def owner(t):
    m, c = t // TILES, t % TILES
    group = (c * LANES + LANES // 2) // GROUP
    second = jnp.where((c == 2) | (c == 6) | (c == 9), 1, 0)
    return lax.rem(group + Z // 2, Z) * Y + 2 * m + second


def tile_of(device):
    group, y = lax.rem(device // Y + Z // 2, Z), lax.rem(device, Y)
    m, second = y // 2, y % 2
    two = (group == 1) | (group == 4) | (group == 6)
    return m * TILES + pick_from(group, (0, 1, 3, 4, 5, 7, 8, 10)) + second, two | (second == 0)


def tiles_of(group):
    return group * GROUP // LANES, (group * GROUP + GROUP - 1) // LANES


def window(j):
    first, last = tiles_of(j // Y)
    base = jnp.minimum(jnp.maximum(j * OWN // LANES, first), last - 1)
    return base, j * OWN - base * LANES


def kernel(
    wg_ref, wu_ref, rw_hbm, gain_hbm,
    og_ref, ou_ref, sg_ref, su_ref, or_ref,
    w, rw, gain, part, sums, total, q, tmp, send, recv, rt, rts, row,
    load_sem, small_sem, rs_send, rs_recv, ag_send, ag_recv, rt_send, rt_recv, x_send, x_recv,
    send_sem, recv_sem,
):
    me = lax.axis_index("shard")
    ex = lax.axis_index("expert")
    z, y = me // Y, me % Y
    mine, owns = tile_of(me)

    def offset(i):
        g = i // Y
        dz = jnp.where(g % 2 == 1, (7 - g) // 2, 4 + g // 2)
        return dz, lax.rem(i + 1, Y)

    def peer(k):
        dz, dy = offset(k - 1)
        return lax.rem(z + dz, Z) * Y + lax.rem(y + dy, Y)

    def across(k):
        return lax.rem(ex + k, GROUPS)

    def loads(m, e):
        ref = wg_ref if m == 0 else wu_ref
        return pltpu.make_async_copy(ref.at[e], w.at[m, e], load_sem.at[m * E + e])

    barrier = pltpu.get_barrier_semaphore()

    def greet(k, _):
        pl.semaphore_signal(barrier, inc=1, device_id={"shard": peer(k)}, device_id_type=MESH)
        return 0

    def greet_across(k, _):
        pl.semaphore_signal(barrier, inc=1, device_id={"expert": across(k)}, device_id_type=MESH)
        return 0

    for m in range(2):
        for e in range(E):
            loads(m, e).start()
    small = (
        pltpu.make_async_copy(rw_hbm, rw, small_sem.at[0]),
        pltpu.make_async_copy(gain_hbm, gain, small_sem.at[1]),
    )
    for copy in small:
        copy.start()
    lax.fori_loop(1, N, greet, 0)
    lax.fori_loop(1, GROUPS, greet_across, 0)

    for copy in small:
        copy.wait()
    routed = (rw[...] * gain[...]).astype(jnp.bfloat16)
    rt[...] = jnp.concatenate([routed, routed], axis=1)

    def sum_of(m):
        def body(e, _):
            pltpu.make_async_copy(wg_ref.at[e], w.at[m, e], load_sem.at[m * E + e]).wait()
            acc = jnp.abs(w[m, e, 0:8, :])
            for g in range(1, ROWS // 8):
                acc = acc + jnp.abs(w[m, e, g * 8 : g * 8 + 8, :])
            part[pl.ds(m * 8 + e, 1), :] = jnp.sum(acc, axis=0, keepdims=True)
            return 0

        lax.fori_loop(0, E, body, 0)

    def rs(k):
        to = peer(k)
        t, has = tile_of(to)
        return has, lambda: pltpu.make_async_remote_copy(
            src_ref=part.at[tile(t)], dst_ref=sums.at[k], send_sem=rs_send.at[k],
            recv_sem=rs_recv.at[k], device_id={"shard": to}, device_id_type=MESH,
        )

    def rs_wait(k):
        pltpu.make_async_copy(sums.at[0], sums.at[k], rs_recv.at[k]).wait()

    def ag(k):
        return pltpu.make_async_remote_copy(
            src_ref=total.at[tile(mine)], dst_ref=total.at[tile(mine)], send_sem=ag_send.at[k],
            recv_sem=ag_recv.at[mine], device_id={"shard": peer(N - k)}, device_id_type=MESH,
        )

    def router(k):
        return pltpu.make_async_remote_copy(
            src_ref=rt, dst_ref=rts.at[me], send_sem=rt_send.at[k],
            recv_sem=rt_recv.at[me], device_id={"shard": peer(k)}, device_id_type=MESH,
        )

    def router_across(k):
        return pltpu.make_async_remote_copy(
            src_ref=row, dst_ref=or_ref.at[ex], send_sem=x_send.at[k],
            recv_sem=x_recv.at[ex], device_id={"expert": across(k)}, device_id_type=MESH,
        )

    def rs_start(m):
        def body(k, _):
            has, copy = rs(k)

            @pl.when(has & (tile_of(peer(k))[0] // TILES == m))
            def _():
                copy().start()

            return 0

        lax.fori_loop(1, N, body, 0)

    sum_of(0)
    pl.semaphore_wait(barrier, N - 1 + GROUPS - 1)
    rs_start(0)
    sum_of(1)
    rs_start(1)
    lax.fori_loop(1, N, lambda k, _: (router(k).start(), 0)[1], 0)

    @pl.when(owns)
    def _():
        def add(k, acc):
            rs_wait(k)
            return acc + sums[k]

        total[tile(mine)] = lax.fori_loop(1, N, add, part[tile(mine)])
        lax.fori_loop(1, N, lambda k, _: (ag(k).start(), 0)[1], 0)

    def scale_tile(m, c):
        cols = pl.ds(pl.multiple_of(c * LANES, LANES), LANES)
        t = m * TILES + c

        @pl.when(owner(t) != me)
        def _():
            pltpu.make_async_copy(part.at[tile(t)], total.at[tile(t)], ag_recv.at[t]).wait()

        inv = D_MODEL / total[m * 8 : m * 8 + 8, cols]
        for e in range(E):
            q[m, e * ROWS : (e + 1) * ROWS, cols] = (
                w[m, e, :, cols] * inv[e : e + 1, :]
            ).astype(jnp.bfloat16)

    def order(i):
        early = i < 3 * Y
        j = i - 3 * Y
        dz = jnp.where(early, pick_from(i % 3, (3, 5, 4)), pick_from(j % 5, (2, 6, 1, 7, 0)))
        return dz, pick_from(jnp.where(early, i // 3, j // 5), (1, 3, 2, 0))

    def bulk(m, i):
        dz, dy = order(i)
        to = lax.rem(z + dz, Z) * Y + lax.rem(y + dy, Y)
        return to, lambda: pltpu.make_async_remote_copy(
            src_ref=send.at[m, to], dst_ref=recv.at[m, me], send_sem=send_sem.at[m, i],
            recv_sem=recv_sem.at[m, me], device_id={"shard": to}, device_id_type=MESH,
        )

    def select(first, x):
        at = lax.broadcasted_iota(jnp.int32, (PAD, 2 * LANES), 0) + first
        pick = (at == lax.broadcasted_iota(jnp.int32, (PAD, 2 * LANES), 1)).astype(jnp.float32)
        return lax.dot_general(
            pick.astype(jnp.bfloat16), x, (((1,), (1,)), ((), ())), preferred_element_type=jnp.float32
        )

    def pack(m, j):
        base, shift = window(j)
        cols = pl.ds(pl.multiple_of(base * LANES, LANES), 2 * LANES)
        for k in range(2):
            x = q[m, k * 4 * ROWS : (k + 1) * 4 * ROWS, cols]
            low, high = select(shift, x), select(shift + HALF, x)
            for e in range(4):
                lanes = slice(e * ROWS, (e + 1) * ROWS)
                tmp[pl.ds(4 * k + e, PAD, stride=8), :] = jnp.concatenate(
                    [low[:, lanes], high[:, lanes]], axis=1
                )
        send[m, j] = tmp[0 : HALF * 8, :].reshape(HALF, 8, LANES).astype(jnp.bfloat16)

    def group_ready(m):
        def body(step, _):
            group = lax.rem(z + offset(step * Y)[0], Z)
            first, last = tiles_of(group)
            below = ((step % 2 == 0) & (step > 0)) | (step == Z - 1)
            above = step % 2 == 1
            first = first + jnp.where(below & (group > 0), 1, 0)
            last = last - jnp.where(above & (group < Z - 1), 1, 0)
            lax.fori_loop(first, last + 1, lambda c, _: (scale_tile(m, c), 0)[1], 0)
            return 0

        return body

    def send_one(m):
        def body(i, _):
            to, copy = bulk(m, i)
            pack(m, to)

            @pl.when(i < N - 1)
            def _():
                copy().start()

            return 0

        return body

    for m in range(2):
        for start, end in ((0, 3), (3, Z)):
            lax.fori_loop(start, end, group_ready(m), 0)
            lax.fori_loop(start * Y, end * Y, send_one(m), 0)
        pltpu.make_async_copy(send.at[m, me], recv.at[m, me], recv_sem.at[m, me]).start()

    base, shift = window(me)
    for m, ref in enumerate((sg_ref, su_ref)):
        rows = pl.ds(m * 8, 8)
        pair = total[rows, pl.ds(pl.multiple_of(base * LANES, LANES), 2 * LANES)]
        ref[...] = pltpu.roll(pair, 2 * LANES - shift, 1)[:, :OWN] / D_MODEL

    low = lax.broadcasted_iota(jnp.int32, (8, LANES), 1) < ROWS
    rts[me] = rt[...]

    def rt_wait(s, _):
        @pl.when(s != me)
        def _():
            pltpu.make_async_remote_copy(
                src_ref=rt, dst_ref=rts.at[s], send_sem=rt_send.at[0],
                recv_sem=rt_recv.at[s], device_id={"shard": me}, device_id_type=MESH,
            ).wait_recv()

        return 0

    lax.fori_loop(0, N, rt_wait, 0)
    for p in range(N // 2):
        a, b = rts[2 * p].astype(jnp.float32), rts[2 * p + 1].astype(jnp.float32)
        row[:, p * LANES : (p + 1) * LANES] = jnp.where(low, a, b).astype(jnp.bfloat16)
    lax.fori_loop(1, GROUPS, lambda k, _: (router_across(k).start(), 0)[1], 0)
    own_row = pltpu.make_async_copy(row, or_ref.at[ex], x_recv.at[ex])
    own_row.start()

    def merge(m, out):
        def body(i, _):
            p = lax.rem(z - offset(i * 2)[0] + Z, Z) * 2 + i % 2
            for h in range(2):
                s = 2 * p + h
                pltpu.make_async_copy(send.at[m, s], recv.at[m, s], recv_sem.at[m, s]).wait()
            a, b = recv[m, 2 * p], recv[m, 2 * p + 1]
            lanes = pl.ds(pl.multiple_of(p * LANES, LANES), LANES)
            out[0:HALF, :, lanes] = jnp.concatenate([a[..., :ROWS], b[..., :ROWS]], axis=-1)
            out[HALF:OWN, :, lanes] = jnp.concatenate([a[..., ROWS:], b[..., ROWS:]], axis=-1)
            return 0

        return body

    lax.fori_loop(0, N // 2, merge(0, og_ref), 0)
    lax.fori_loop(0, N // 2, merge(1, ou_ref), 0)

    def drain(i, _):
        bulk(0, i)[1]().wait_send()
        bulk(1, i)[1]().wait_send()
        router(i + 1).wait_send()
        has, copy = rs(i + 1)

        @pl.when(has)
        def _():
            copy().wait_send()

        @pl.when(owns)
        def _():
            ag(i + 1).wait_send()

        return 0

    lax.fori_loop(0, N - 1, drain, 0)
    lax.fori_loop(1, GROUPS, lambda k, _: (router_across(k).wait_send(), 0)[1], 0)

    def x_wait(k, _):
        pltpu.make_async_copy(row, or_ref.at[k], x_recv.at[k]).wait()
        return 0

    lax.fori_loop(0, GROUPS, x_wait, 0)


def put_out(*refs):
    ins, outs, sem = refs[:5], refs[5:10], refs[10]
    copies = [pltpu.make_async_copy(a, b, sem.at[i]) for i, (a, b) in enumerate(zip(ins, outs))]
    for copy in copies:
        copy.start()
    for copy in copies:
        copy.wait()


def on_device(w_gate, w_up, router_weight, router_gain):
    any_ = pl.BlockSpec(memory_space=pl.ANY)
    hbm = pl.BlockSpec(memory_space=pltpu.HBM)
    vmem = pl.BlockSpec(memory_space=pltpu.VMEM)
    dma = pltpu.SemaphoreType.DMA
    bf16, f32 = jnp.bfloat16, jnp.float32
    results = (
        jax.ShapeDtypeStruct((OWN, E, D_MODEL), bf16),
        jax.ShapeDtypeStruct((OWN, E, D_MODEL), bf16),
        jax.ShapeDtypeStruct((E, OWN), f32),
        jax.ShapeDtypeStruct((E, OWN), f32),
        jax.ShapeDtypeStruct((GROUPS, 8, D_MODEL), bf16),
    )
    held = pl.pallas_call(
        kernel,
        out_shape=results,
        in_specs=[hbm] * 4,
        out_specs=(vmem,) * 5,
        scratch_shapes=[
            pltpu.VMEM((2, E, ROWS, COLS), f32),
            pltpu.VMEM((8, ROWS), f32),
            pltpu.VMEM((1, ROWS), f32),
            pltpu.VMEM((16, COLS), f32),
            pltpu.VMEM((N, 8, LANES), f32),
            pltpu.VMEM((16, COLS), f32),
            pltpu.VMEM((2, E * ROWS, COLS), bf16),
            pltpu.VMEM((PAD * 8, LANES), f32),
            pltpu.VMEM((2, N, HALF, 8, LANES), bf16),
            pltpu.VMEM((2, N, HALF, 8, LANES), bf16),
            pltpu.VMEM((8, LANES), bf16),
            pltpu.VMEM((N, 8, LANES), bf16),
            pltpu.VMEM((8, D_MODEL), bf16),
            dma((2 * E,)), dma((2,)), dma((N,)), dma((N,)), dma((N,)), dma((N,)), dma((N,)), dma((N,)),
            dma((GROUPS,)), dma((GROUPS,)), dma((2, N)), dma((2, N)),
        ],
        compiler_params=pltpu.CompilerParams(
            collective_id=0, has_side_effects=True, vmem_limit_bytes=48 << 20
        ),
    )(*(
        pltpu.with_memory_space_constraint(x, pltpu.HBM)
        for x in (w_gate, w_up, router_weight.T, router_gain[None, :])
    ))
    gate, up, scale_gate, scale_up, router = pl.pallas_call(
        put_out,
        out_shape=results,
        in_specs=[any_] * 5,
        out_specs=(any_,) * 5,
        scratch_shapes=[dma((5,))],
    )(*(pltpu.with_memory_space_constraint(x, pltpu.VMEM) for x in held))
    return (
        gate.transpose(1, 2, 0),
        up.transpose(1, 2, 0),
        scale_gate,
        scale_up,
        router.reshape(GROUPS * 8, D_MODEL).T,
    )


def solution(mesh):
    placed = (
        P("expert", "shard", None),
        P("expert", "shard", None),
        P("shard", "expert"),
        P("shard"),
    )
    return jax.shard_map(
        on_device,
        mesh=mesh,
        in_specs=placed,
        out_specs=(
            P("expert", None, "shard"),
            P("expert", None, "shard"),
            P("expert", "shard"),
            P("expert", "shard"),
            P(),
        ),
        check_vma=False,
    )
```

```python
import functools

import jax
import jax.numpy as jnp
from jax import lax
from jax.experimental import pallas as pl
from jax.experimental.pallas import tpu as pltpu
from jax.sharding import PartitionSpec as P

MESH = pl.DeviceIdType.MESH
Z, Y = 8, 4
N = Z * Y
GROUPS = 8
E, ROWS, COLS = 8, 64, 1408
D_MODEL = N * ROWS
OWN = COLS // N
HALF, PAD = OWN // 2, 24
LANES = 128
TILES = COLS // LANES
GROUP = Y * OWN


def tile(t):
    m, c = t // TILES, t % TILES
    return (
        pl.ds(pl.multiple_of(m * 8, 8), 8),
        pl.ds(pl.multiple_of(c * LANES, LANES), LANES),
    )


def pick_from(i, values):
    chosen = values[0]
    for at, value in enumerate(values[1:], 1):
        chosen = jnp.where(i == at, value, chosen)
    return chosen


def owner(t):
    m, c = t // TILES, t % TILES
    group = (c * LANES + LANES // 2) // GROUP
    second = jnp.where((c == 2) | (c == 6) | (c == 9), 1, 0)
    return lax.rem(group + Z // 2, Z) * Y + 2 * m + second


def tile_of(device):
    group, y = lax.rem(device // Y + Z // 2, Z), lax.rem(device, Y)
    m, second = y // 2, y % 2
    two = (group == 1) | (group == 4) | (group == 6)
    return m * TILES + pick_from(group, (0, 1, 3, 4, 5, 7, 8, 10)) + second, two | (second == 0)


def tiles_of(group):
    return group * GROUP // LANES, (group * GROUP + GROUP - 1) // LANES


def window(j):
    first, last = tiles_of(j // Y)
    base = jnp.minimum(jnp.maximum(j * OWN // LANES, first), last - 1)
    return base, j * OWN - base * LANES


def kernel(
    wg_ref, wu_ref, rw_hbm, gain_hbm,
    og_ref, ou_ref, sg_ref, su_ref, or_ref,
    w, rw, gain, part, sums, total, q, tmp, send, recv, rt, rts, row,
    load_sem, small_sem, rs_send, rs_recv, ag_send, ag_recv, rt_send, rt_recv, x_send, x_recv,
    send_sem, recv_sem,
):
    me = lax.axis_index("shard")
    ex = lax.axis_index("expert")
    z, y = me // Y, me % Y
    mine, owns = tile_of(me)

    def offset(i):
        g = i // Y
        dz = jnp.where(g % 2 == 1, (7 - g) // 2, 4 + g // 2)
        return dz, lax.rem(i + 1, Y)

    def peer(k):
        dz, dy = offset(k - 1)
        return lax.rem(z + dz, Z) * Y + lax.rem(y + dy, Y)

    def across(k):
        return lax.rem(ex + k, GROUPS)

    def loads(m, e):
        ref = wg_ref if m == 0 else wu_ref
        return pltpu.make_async_copy(ref.at[e], w.at[m, e], load_sem.at[m * E + e])

    barrier = pltpu.get_barrier_semaphore()

    def greet(k, _):
        pl.semaphore_signal(barrier, inc=1, device_id={"shard": peer(k)}, device_id_type=MESH)
        return 0

    def greet_across(k, _):
        pl.semaphore_signal(barrier, inc=1, device_id={"expert": across(k)}, device_id_type=MESH)
        return 0

    for m in range(2):
        for e in range(E):
            loads(m, e).start()
    small = (
        pltpu.make_async_copy(rw_hbm, rw, small_sem.at[0]),
        pltpu.make_async_copy(gain_hbm, gain, small_sem.at[1]),
    )
    for copy in small:
        copy.start()
    lax.fori_loop(1, N, greet, 0)
    lax.fori_loop(1, GROUPS, greet_across, 0)

    for copy in small:
        copy.wait()
    routed = (rw[...] * gain[...]).astype(jnp.bfloat16)
    rt[...] = jnp.concatenate([routed, routed], axis=1)

    def sum_of(m):
        def body(e, _):
            pltpu.make_async_copy(wg_ref.at[e], w.at[m, e], load_sem.at[m * E + e]).wait()
            acc = jnp.abs(w[m, e, 0:8, :])
            for g in range(1, ROWS // 8):
                acc = acc + jnp.abs(w[m, e, g * 8 : g * 8 + 8, :])
            part[pl.ds(m * 8 + e, 1), :] = jnp.sum(acc, axis=0, keepdims=True)
            return 0

        lax.fori_loop(0, E, body, 0)

    def rs(k):
        to = peer(k)
        t, has = tile_of(to)
        return has, lambda: pltpu.make_async_remote_copy(
            src_ref=part.at[tile(t)], dst_ref=sums.at[k], send_sem=rs_send.at[k],
            recv_sem=rs_recv.at[k], device_id={"shard": to}, device_id_type=MESH,
        )

    def rs_wait(k):
        pltpu.make_async_copy(sums.at[0], sums.at[k], rs_recv.at[k]).wait()

    def ag(k):
        return pltpu.make_async_remote_copy(
            src_ref=total.at[tile(mine)], dst_ref=total.at[tile(mine)], send_sem=ag_send.at[k],
            recv_sem=ag_recv.at[mine], device_id={"shard": peer(N - k)}, device_id_type=MESH,
        )

    def router(k):
        return pltpu.make_async_remote_copy(
            src_ref=rt, dst_ref=rts.at[me], send_sem=rt_send.at[k],
            recv_sem=rt_recv.at[me], device_id={"shard": peer(k)}, device_id_type=MESH,
        )

    def router_across(k):
        return pltpu.make_async_remote_copy(
            src_ref=row, dst_ref=or_ref.at[ex], send_sem=x_send.at[k],
            recv_sem=x_recv.at[ex], device_id={"expert": across(k)}, device_id_type=MESH,
        )

    def rs_start(m):
        def body(k, _):
            has, copy = rs(k)

            @pl.when(has & (tile_of(peer(k))[0] // TILES == m))
            def _():
                copy().start()

            return 0

        lax.fori_loop(1, N, body, 0)

    sum_of(0)
    pl.semaphore_wait(barrier, N - 1 + GROUPS - 1)
    rs_start(0)
    sum_of(1)
    rs_start(1)
    lax.fori_loop(1, N, lambda k, _: (router(k).start(), 0)[1], 0)

    @pl.when(owns)
    def _():
        def add(k, acc):
            rs_wait(k)
            return acc + sums[k]

        total[tile(mine)] = lax.fori_loop(1, N, add, part[tile(mine)])
        lax.fori_loop(1, N, lambda k, _: (ag(k).start(), 0)[1], 0)

    def scale_tile(m, c):
        cols = pl.ds(pl.multiple_of(c * LANES, LANES), LANES)
        t = m * TILES + c

        @pl.when(owner(t) != me)
        def _():
            pltpu.make_async_copy(part.at[tile(t)], total.at[tile(t)], ag_recv.at[t]).wait()

        inv = D_MODEL / total[m * 8 : m * 8 + 8, cols]
        for e in range(E):
            q[m, e * ROWS : (e + 1) * ROWS, cols] = (
                w[m, e, :, cols] * inv[e : e + 1, :]
            ).astype(jnp.bfloat16)

    def order(i):
        early = i < 3 * Y
        j = i - 3 * Y
        dz = jnp.where(early, pick_from(i % 3, (3, 5, 4)), pick_from(j % 5, (2, 6, 1, 7, 0)))
        return dz, pick_from(jnp.where(early, i // 3, j // 5), (1, 3, 2, 0))

    def bulk(m, i):
        dz, dy = order(i)
        to = lax.rem(z + dz, Z) * Y + lax.rem(y + dy, Y)
        return to, lambda: pltpu.make_async_remote_copy(
            src_ref=send.at[m, to], dst_ref=recv.at[m, me], send_sem=send_sem.at[m, i],
            recv_sem=recv_sem.at[m, me], device_id={"shard": to}, device_id_type=MESH,
        )

    def select(first, x):
        at = lax.broadcasted_iota(jnp.int32, (PAD, 2 * LANES), 0) + first
        pick = (at == lax.broadcasted_iota(jnp.int32, (PAD, 2 * LANES), 1)).astype(jnp.float32)
        return lax.dot_general(
            pick.astype(jnp.bfloat16), x, (((1,), (1,)), ((), ())), preferred_element_type=jnp.float32
        )

    def pack(m, j):
        base, shift = window(j)
        cols = pl.ds(pl.multiple_of(base * LANES, LANES), 2 * LANES)
        for k in range(2):
            x = q[m, k * 4 * ROWS : (k + 1) * 4 * ROWS, cols]
            low, high = select(shift, x), select(shift + HALF, x)
            for e in range(4):
                lanes = slice(e * ROWS, (e + 1) * ROWS)
                tmp[pl.ds(4 * k + e, PAD, stride=8), :] = jnp.concatenate(
                    [low[:, lanes], high[:, lanes]], axis=1
                )
        send[m, j] = tmp[0 : HALF * 8, :].reshape(HALF, 8, LANES).astype(jnp.bfloat16)

    def group_ready(m):
        def body(step, _):
            group = lax.rem(z + offset(step * Y)[0], Z)
            first, last = tiles_of(group)
            below = ((step % 2 == 0) & (step > 0)) | (step == Z - 1)
            above = step % 2 == 1
            first = first + jnp.where(below & (group > 0), 1, 0)
            last = last - jnp.where(above & (group < Z - 1), 1, 0)
            lax.fori_loop(first, last + 1, lambda c, _: (scale_tile(m, c), 0)[1], 0)
            return 0

        return body

    def send_one(m):
        def body(i, _):
            to, copy = bulk(m, i)
            pack(m, to)

            @pl.when(i < N - 1)
            def _():
                copy().start()

            return 0

        return body

    for m in range(2):
        for start, end in ((0, 3), (3, Z)):
            lax.fori_loop(start, end, group_ready(m), 0)
            lax.fori_loop(start * Y, end * Y, send_one(m), 0)
        pltpu.make_async_copy(send.at[m, me], recv.at[m, me], recv_sem.at[m, me]).start()

    base, shift = window(me)
    for m, ref in enumerate((sg_ref, su_ref)):
        rows = pl.ds(m * 8, 8)
        pair = total[rows, pl.ds(pl.multiple_of(base * LANES, LANES), 2 * LANES)]
        ref[...] = pltpu.roll(pair, 2 * LANES - shift, 1)[:, :OWN] / D_MODEL

    low = lax.broadcasted_iota(jnp.int32, (8, LANES), 1) < ROWS
    rts[me] = rt[...]

    def rt_wait(s, _):
        @pl.when(s != me)
        def _():
            pltpu.make_async_remote_copy(
                src_ref=rt, dst_ref=rts.at[s], send_sem=rt_send.at[0],
                recv_sem=rt_recv.at[s], device_id={"shard": me}, device_id_type=MESH,
            ).wait_recv()

        return 0

    lax.fori_loop(0, N, rt_wait, 0)
    for p in range(N // 2):
        a, b = rts[2 * p].astype(jnp.float32), rts[2 * p + 1].astype(jnp.float32)
        row[:, p * LANES : (p + 1) * LANES] = jnp.where(low, a, b).astype(jnp.bfloat16)
    lax.fori_loop(1, GROUPS, lambda k, _: (router_across(k).start(), 0)[1], 0)
    own_row = pltpu.make_async_copy(row, or_ref.at[ex], x_recv.at[ex])
    own_row.start()

    def merge(m, out):
        def body(i, _):
            p = lax.rem(z - offset(i * 2)[0] + Z, Z) * 2 + i % 2
            for h in range(2):
                s = 2 * p + h
                pltpu.make_async_copy(send.at[m, s], recv.at[m, s], recv_sem.at[m, s]).wait()
            a, b = recv[m, 2 * p], recv[m, 2 * p + 1]
            lanes = pl.ds(pl.multiple_of(p * LANES, LANES), LANES)
            out[0:HALF, :, lanes] = jnp.concatenate([a[..., :ROWS], b[..., :ROWS]], axis=-1)
            out[HALF:OWN, :, lanes] = jnp.concatenate([a[..., ROWS:], b[..., ROWS:]], axis=-1)
            return 0

        return body

    def sent(m, i):
        pltpu.make_async_copy(send.at[m, 0], recv.at[m, 0], send_sem.at[m, i]).wait()
        return 0

    def drain(i, _):
        sent(0, i)
        router(i + 1).wait_send()
        has, copy = rs(i + 1)

        @pl.when(has)
        def _():
            copy().wait_send()

        @pl.when(owns)
        def _():
            ag(i + 1).wait_send()

        return 0

    lax.fori_loop(0, N - 1, drain, 0)
    lax.fori_loop(1, GROUPS, lambda k, _: (router_across(k).wait_send(), 0)[1], 0)

    def x_wait(k, _):
        pltpu.make_async_copy(row, or_ref.at[k], x_recv.at[k]).wait()
        return 0

    lax.fori_loop(0, GROUPS, x_wait, 0)

    lax.fori_loop(0, N // 2, merge(0, og_ref), 0)
    lax.fori_loop(0, N - 1, lambda i, _: sent(1, i), 0)
    lax.fori_loop(0, N // 2, merge(1, ou_ref), 0)


def put_out(*refs):
    ins, outs, sem = refs[:5], refs[5:10], refs[10]
    copies = [pltpu.make_async_copy(a, b, sem.at[i]) for i, (a, b) in enumerate(zip(ins, outs))]
    for copy in copies:
        copy.start()
    for copy in copies:
        copy.wait()


def on_device(w_gate, w_up, router_weight, router_gain):
    any_ = pl.BlockSpec(memory_space=pl.ANY)
    hbm = pl.BlockSpec(memory_space=pltpu.HBM)
    vmem = pl.BlockSpec(memory_space=pltpu.VMEM)
    dma = pltpu.SemaphoreType.DMA
    bf16, f32 = jnp.bfloat16, jnp.float32
    results = (
        jax.ShapeDtypeStruct((OWN, E, D_MODEL), bf16),
        jax.ShapeDtypeStruct((OWN, E, D_MODEL), bf16),
        jax.ShapeDtypeStruct((E, OWN), f32),
        jax.ShapeDtypeStruct((E, OWN), f32),
        jax.ShapeDtypeStruct((GROUPS, 8, D_MODEL), bf16),
    )
    held = pl.pallas_call(
        kernel,
        out_shape=results,
        in_specs=[hbm] * 4,
        out_specs=(vmem,) * 5,
        scratch_shapes=[
            pltpu.VMEM((2, E, ROWS, COLS), f32),
            pltpu.VMEM((8, ROWS), f32),
            pltpu.VMEM((1, ROWS), f32),
            pltpu.VMEM((16, COLS), f32),
            pltpu.VMEM((N, 8, LANES), f32),
            pltpu.VMEM((16, COLS), f32),
            pltpu.VMEM((2, E * ROWS, COLS), bf16),
            pltpu.VMEM((PAD * 8, LANES), f32),
            pltpu.VMEM((2, N, HALF, 8, LANES), bf16),
            pltpu.VMEM((2, N, HALF, 8, LANES), bf16),
            pltpu.VMEM((8, LANES), bf16),
            pltpu.VMEM((N, 8, LANES), bf16),
            pltpu.VMEM((8, D_MODEL), bf16),
            dma((2 * E,)), dma((2,)), dma((N,)), dma((N,)), dma((N,)), dma((N,)), dma((N,)), dma((N,)),
            dma((GROUPS,)), dma((GROUPS,)), dma((2, N)), dma((2, N)),
        ],
        compiler_params=pltpu.CompilerParams(
            collective_id=0, has_side_effects=True, vmem_limit_bytes=48 << 20
        ),
    )(*(
        pltpu.with_memory_space_constraint(x, pltpu.HBM)
        for x in (w_gate, w_up, router_weight.T, router_gain[None, :])
    ))
    gate, up, scale_gate, scale_up, router = pl.pallas_call(
        put_out,
        out_shape=results,
        in_specs=[any_] * 5,
        out_specs=(any_,) * 5,
        scratch_shapes=[dma((5,))],
    )(*(pltpu.with_memory_space_constraint(x, pltpu.VMEM) for x in held))
    return (
        gate.transpose(1, 2, 0),
        up.transpose(1, 2, 0),
        scale_gate,
        scale_up,
        router.reshape(GROUPS * 8, D_MODEL).T,
    )


def solution(mesh):
    placed = (
        P("expert", "shard", None),
        P("expert", "shard", None),
        P("shard", "expert"),
        P("shard"),
    )
    return jax.shard_map(
        on_device,
        mesh=mesh,
        in_specs=placed,
        out_specs=(
            P("expert", None, "shard"),
            P("expert", None, "shard"),
            P("expert", "shard"),
            P("expert", "shard"),
            P(),
        ),
        check_vma=False,
    )
```

```python
import functools

import jax
import jax.numpy as jnp
from jax import lax
from jax.experimental import pallas as pl
from jax.experimental.pallas import tpu as pltpu
from jax.sharding import PartitionSpec as P

MESH = pl.DeviceIdType.MESH
Z, Y = 8, 4
N = Z * Y
GROUPS = 8
E, ROWS, COLS = 8, 64, 1408
D_MODEL = N * ROWS
OWN = COLS // N
HALF, PAD = OWN // 2, 24
LANES = 128
TILES = COLS // LANES
GROUP = Y * OWN


def tile(t):
    m, c = t // TILES, t % TILES
    return (
        pl.ds(pl.multiple_of(m * 8, 8), 8),
        pl.ds(pl.multiple_of(c * LANES, LANES), LANES),
    )


def pick_from(i, values):
    chosen = values[0]
    for at, value in enumerate(values[1:], 1):
        chosen = jnp.where(i == at, value, chosen)
    return chosen


def owner(t):
    m, c = t // TILES, t % TILES
    group = (c * LANES + LANES // 2) // GROUP
    second = jnp.where((c == 2) | (c == 6) | (c == 9), 1, 0)
    return lax.rem(group + Z // 2, Z) * Y + 2 * m + second


def tile_of(device):
    group, y = lax.rem(device // Y + Z // 2, Z), lax.rem(device, Y)
    m, second = y // 2, y % 2
    two = (group == 1) | (group == 4) | (group == 6)
    return m * TILES + pick_from(group, (0, 1, 3, 4, 5, 7, 8, 10)) + second, two | (second == 0)


def tiles_of(group):
    return group * GROUP // LANES, (group * GROUP + GROUP - 1) // LANES


def window(j):
    first, last = tiles_of(j // Y)
    base = jnp.minimum(jnp.maximum(j * OWN // LANES, first), last - 1)
    return base, j * OWN - base * LANES


def kernel(
    wg_ref, wu_ref, rw_hbm, gain_hbm,
    og_ref, ou_ref, sg_ref, su_ref, or_ref,
    w, rw, gain, part, sums, total, q, tmp, send, recv, rt, rts, row,
    load_sem, small_sem, rs_send, rs_recv, ag_send, ag_recv, rt_send, rt_recv, x_send, x_recv,
    send_sem, recv_sem,
):
    me = lax.axis_index("shard")
    ex = lax.axis_index("expert")
    z, y = me // Y, me % Y
    mine, owns = tile_of(me)

    def offset(i):
        if isinstance(i, int):
            g = i // Y
            return (7 - g) // 2 if g % 2 else 4 + g // 2, (i + 1) % Y
        g = i // Y
        dz = jnp.where(g % 2 == 1, (7 - g) // 2, 4 + g // 2)
        return dz, lax.rem(i + 1, Y)

    def peer(k):
        dz, dy = offset(k - 1)
        return lax.rem(z + dz, Z) * Y + lax.rem(y + dy, Y)

    def across(k):
        return lax.rem(ex + k, GROUPS)

    def loads(m, e):
        ref = wg_ref if m == 0 else wu_ref
        return pltpu.make_async_copy(ref.at[e], w.at[m, e], load_sem.at[m * E + e])

    barrier = pltpu.get_barrier_semaphore()

    def greet(k, _):
        pl.semaphore_signal(barrier, inc=1, device_id={"shard": peer(k)}, device_id_type=MESH)
        return 0

    def greet_across(k, _):
        pl.semaphore_signal(barrier, inc=1, device_id={"expert": across(k)}, device_id_type=MESH)
        return 0

    for m in range(2):
        for e in range(E):
            loads(m, e).start()
    small = (
        pltpu.make_async_copy(rw_hbm, rw, small_sem.at[0]),
        pltpu.make_async_copy(gain_hbm, gain, small_sem.at[1]),
    )
    for copy in small:
        copy.start()
    lax.fori_loop(1, N, greet, 0)
    lax.fori_loop(1, GROUPS, greet_across, 0)

    for copy in small:
        copy.wait()
    routed = (rw[...] * gain[...]).astype(jnp.bfloat16)
    rt[...] = jnp.concatenate([routed, routed], axis=1)

    def sum_of(m):
        def body(e, _):
            pltpu.make_async_copy(wg_ref.at[e], w.at[m, e], load_sem.at[m * E + e]).wait()
            acc = jnp.abs(w[m, e, 0:8, :])
            for g in range(1, ROWS // 8):
                acc = acc + jnp.abs(w[m, e, g * 8 : g * 8 + 8, :])
            part[pl.ds(m * 8 + e, 1), :] = jnp.sum(acc, axis=0, keepdims=True)
            return 0

        lax.fori_loop(0, E, body, 0)

    def rs(k):
        to = peer(k)
        t, has = tile_of(to)
        return has, lambda: pltpu.make_async_remote_copy(
            src_ref=part.at[tile(t)], dst_ref=sums.at[k], send_sem=rs_send.at[k],
            recv_sem=rs_recv.at[k], device_id={"shard": to}, device_id_type=MESH,
        )

    def rs_wait(k):
        pltpu.make_async_copy(sums.at[0], sums.at[k], rs_recv.at[k]).wait()

    def ag(k):
        return pltpu.make_async_remote_copy(
            src_ref=total.at[tile(mine)], dst_ref=total.at[tile(mine)], send_sem=ag_send.at[k],
            recv_sem=ag_recv.at[mine], device_id={"shard": peer(N - k)}, device_id_type=MESH,
        )

    def router(k):
        return pltpu.make_async_remote_copy(
            src_ref=rt, dst_ref=rts.at[me], send_sem=rt_send.at[k],
            recv_sem=rt_recv.at[me], device_id={"shard": peer(k)}, device_id_type=MESH,
        )

    def router_across(k):
        return pltpu.make_async_remote_copy(
            src_ref=row, dst_ref=or_ref.at[ex], send_sem=x_send.at[k],
            recv_sem=x_recv.at[ex], device_id={"expert": across(k)}, device_id_type=MESH,
        )

    def rs_start(m):
        def body(k, _):
            has, copy = rs(k)

            @pl.when(has & (tile_of(peer(k))[0] // TILES == m))
            def _():
                copy().start()

            return 0

        for k in range(1, N):
            body(k, 0)

    sum_of(0)
    pl.semaphore_wait(barrier, N - 1 + GROUPS - 1)
    rs_start(0)
    sum_of(1)
    rs_start(1)
    lax.fori_loop(1, N, lambda k, _: (router(k).start(), 0)[1], 0)

    @pl.when(owns)
    def _():
        def add(k, acc):
            rs_wait(k)
            return acc + sums[k]

        total[tile(mine)] = lax.fori_loop(1, N, add, part[tile(mine)])
        for k in range(1, N):
            ag(k).start()

    def scale_tile(m, c):
        cols = pl.ds(pl.multiple_of(c * LANES, LANES), LANES)
        t = m * TILES + c

        @pl.when(owner(t) != me)
        def _():
            pltpu.make_async_copy(part.at[tile(t)], total.at[tile(t)], ag_recv.at[t]).wait()

        inv = D_MODEL / total[m * 8 : m * 8 + 8, cols]
        for e in range(E):
            q[m, e * ROWS : (e + 1) * ROWS, cols] = (
                w[m, e, :, cols] * inv[e : e + 1, :]
            ).astype(jnp.bfloat16)

    def order(i):
        early = i < 3 * Y
        j = i - 3 * Y
        dz = jnp.where(early, pick_from(i % 3, (3, 5, 4)), pick_from(j % 5, (2, 6, 1, 7, 0)))
        return dz, pick_from(jnp.where(early, i // 3, j // 5), (1, 3, 2, 0))

    def bulk(m, i):
        dz, dy = order(i)
        to = lax.rem(z + dz, Z) * Y + lax.rem(y + dy, Y)
        return to, lambda: pltpu.make_async_remote_copy(
            src_ref=send.at[m, to], dst_ref=recv.at[m, me], send_sem=send_sem.at[m, i],
            recv_sem=recv_sem.at[m, me], device_id={"shard": to}, device_id_type=MESH,
        )

    def select(first, x):
        at = lax.broadcasted_iota(jnp.int32, (PAD, 2 * LANES), 0) + first
        pick = (at == lax.broadcasted_iota(jnp.int32, (PAD, 2 * LANES), 1)).astype(jnp.float32)
        return lax.dot_general(
            pick.astype(jnp.bfloat16), x, (((1,), (1,)), ((), ())), preferred_element_type=jnp.float32
        )

    def pack(m, j):
        base, shift = window(j)
        cols = pl.ds(pl.multiple_of(base * LANES, LANES), 2 * LANES)
        for k in range(2):
            x = q[m, k * 4 * ROWS : (k + 1) * 4 * ROWS, cols]
            low, high = select(shift, x), select(shift + HALF, x)
            for e in range(4):
                lanes = slice(e * ROWS, (e + 1) * ROWS)
                tmp[pl.ds(4 * k + e, PAD, stride=8), :] = jnp.concatenate(
                    [low[:, lanes], high[:, lanes]], axis=1
                )
        send[m, j] = tmp[0 : HALF * 8, :].reshape(HALF, 8, LANES).astype(jnp.bfloat16)

    def group_ready(m):
        def body(step, _):
            group = lax.rem(z + offset(step * Y)[0], Z)
            first, last = tiles_of(group)
            below = ((step % 2 == 0) & (step > 0)) | (step == Z - 1)
            above = step % 2 == 1
            first = first + jnp.where(below & (group > 0), 1, 0)
            last = last - jnp.where(above & (group < Z - 1), 1, 0)
            lax.fori_loop(first, last + 1, lambda c, _: (scale_tile(m, c), 0)[1], 0)
            return 0

        return body

    def send_one(m):
        def body(i, _):
            to, copy = bulk(m, i)
            pack(m, to)

            @pl.when(i < N - 1)
            def _():
                copy().start()

            return 0

        return body

    for m in range(2):
        for start, end in ((0, 3), (3, Z)):
            lax.fori_loop(start, end, group_ready(m), 0)
            lax.fori_loop(start * Y, end * Y, send_one(m), 0)
        pltpu.make_async_copy(send.at[m, me], recv.at[m, me], recv_sem.at[m, me]).start()

    base, shift = window(me)
    for m, ref in enumerate((sg_ref, su_ref)):
        rows = pl.ds(m * 8, 8)
        pair = total[rows, pl.ds(pl.multiple_of(base * LANES, LANES), 2 * LANES)]
        ref[...] = pltpu.roll(pair, 2 * LANES - shift, 1)[:, :OWN] / D_MODEL

    low = lax.broadcasted_iota(jnp.int32, (8, LANES), 1) < ROWS
    rts[me] = rt[...]

    def rt_wait(s, _):
        @pl.when(s != me)
        def _():
            pltpu.make_async_remote_copy(
                src_ref=rt, dst_ref=rts.at[s], send_sem=rt_send.at[0],
                recv_sem=rt_recv.at[s], device_id={"shard": me}, device_id_type=MESH,
            ).wait_recv()

        return 0

    lax.fori_loop(0, N, rt_wait, 0)
    for p in range(N // 2):
        a, b = rts[2 * p].astype(jnp.float32), rts[2 * p + 1].astype(jnp.float32)
        row[:, p * LANES : (p + 1) * LANES] = jnp.where(low, a, b).astype(jnp.bfloat16)
    lax.fori_loop(1, GROUPS, lambda k, _: (router_across(k).start(), 0)[1], 0)
    own_row = pltpu.make_async_copy(row, or_ref.at[ex], x_recv.at[ex])
    own_row.start()

    def merge(m, out):
        def body(i, _):
            p = lax.rem(z - offset(i * 2)[0] + Z, Z) * 2 + i % 2
            for h in range(2):
                s = 2 * p + h
                pltpu.make_async_copy(send.at[m, s], recv.at[m, s], recv_sem.at[m, s]).wait()
            a, b = recv[m, 2 * p], recv[m, 2 * p + 1]
            lanes = pl.ds(pl.multiple_of(p * LANES, LANES), LANES)
            out[0:HALF, :, lanes] = jnp.concatenate([a[..., :ROWS], b[..., :ROWS]], axis=-1)
            out[HALF:OWN, :, lanes] = jnp.concatenate([a[..., ROWS:], b[..., ROWS:]], axis=-1)
            return 0

        return body

    def sent(m, i):
        pltpu.make_async_copy(send.at[m, 0], recv.at[m, 0], send_sem.at[m, i]).wait()
        return 0

    def drain(i, _):
        sent(0, i)
        router(i + 1).wait_send()
        has, copy = rs(i + 1)

        @pl.when(has)
        def _():
            copy().wait_send()

        @pl.when(owns)
        def _():
            ag(i + 1).wait_send()

        return 0

    lax.fori_loop(0, N - 1, drain, 0)
    lax.fori_loop(1, GROUPS, lambda k, _: (router_across(k).wait_send(), 0)[1], 0)

    def x_wait(k, _):
        pltpu.make_async_copy(row, or_ref.at[k], x_recv.at[k]).wait()
        return 0

    lax.fori_loop(0, GROUPS, x_wait, 0)

    lax.fori_loop(0, N // 2, merge(0, og_ref), 0)
    lax.fori_loop(0, N - 1, lambda i, _: sent(1, i), 0)
    lax.fori_loop(0, N // 2, merge(1, ou_ref), 0)


def put_out(*refs):
    ins, outs, sem = refs[:5], refs[5:10], refs[10]
    copies = [pltpu.make_async_copy(a, b, sem.at[i]) for i, (a, b) in enumerate(zip(ins, outs))]
    for copy in copies:
        copy.start()
    for copy in copies:
        copy.wait()


def on_device(w_gate, w_up, router_weight, router_gain):
    any_ = pl.BlockSpec(memory_space=pl.ANY)
    hbm = pl.BlockSpec(memory_space=pltpu.HBM)
    vmem = pl.BlockSpec(memory_space=pltpu.VMEM)
    dma = pltpu.SemaphoreType.DMA
    bf16, f32 = jnp.bfloat16, jnp.float32
    results = (
        jax.ShapeDtypeStruct((OWN, E, D_MODEL), bf16),
        jax.ShapeDtypeStruct((OWN, E, D_MODEL), bf16),
        jax.ShapeDtypeStruct((E, OWN), f32),
        jax.ShapeDtypeStruct((E, OWN), f32),
        jax.ShapeDtypeStruct((GROUPS, 8, D_MODEL), bf16),
    )
    held = pl.pallas_call(
        kernel,
        out_shape=results,
        in_specs=[hbm] * 4,
        out_specs=(vmem,) * 5,
        scratch_shapes=[
            pltpu.VMEM((2, E, ROWS, COLS), f32),
            pltpu.VMEM((8, ROWS), f32),
            pltpu.VMEM((1, ROWS), f32),
            pltpu.VMEM((16, COLS), f32),
            pltpu.VMEM((N, 8, LANES), f32),
            pltpu.VMEM((16, COLS), f32),
            pltpu.VMEM((2, E * ROWS, COLS), bf16),
            pltpu.VMEM((PAD * 8, LANES), f32),
            pltpu.VMEM((2, N, HALF, 8, LANES), bf16),
            pltpu.VMEM((2, N, HALF, 8, LANES), bf16),
            pltpu.VMEM((8, LANES), bf16),
            pltpu.VMEM((N, 8, LANES), bf16),
            pltpu.VMEM((8, D_MODEL), bf16),
            dma((2 * E,)), dma((2,)), dma((N,)), dma((N,)), dma((N,)), dma((N,)), dma((N,)), dma((N,)),
            dma((GROUPS,)), dma((GROUPS,)), dma((2, N)), dma((2, N)),
        ],
        compiler_params=pltpu.CompilerParams(
            collective_id=0, has_side_effects=True, vmem_limit_bytes=48 << 20
        ),
    )(*(
        pltpu.with_memory_space_constraint(x, pltpu.HBM)
        for x in (w_gate, w_up, router_weight.T, router_gain[None, :])
    ))
    gate, up, scale_gate, scale_up, router = pl.pallas_call(
        put_out,
        out_shape=results,
        in_specs=[any_] * 5,
        out_specs=(any_,) * 5,
        scratch_shapes=[dma((5,))],
    )(*(pltpu.with_memory_space_constraint(x, pltpu.VMEM) for x in held))
    return (
        gate.transpose(1, 2, 0),
        up.transpose(1, 2, 0),
        scale_gate,
        scale_up,
        router.reshape(GROUPS * 8, D_MODEL).T,
    )


def solution(mesh):
    placed = (
        P("expert", "shard", None),
        P("expert", "shard", None),
        P("shard", "expert"),
        P("shard"),
    )
    return jax.shard_map(
        on_device,
        mesh=mesh,
        in_specs=placed,
        out_specs=(
            P("expert", None, "shard"),
            P("expert", None, "shard"),
            P("expert", "shard"),
            P("expert", "shard"),
            P(),
        ),
        check_vma=False,
    )
```
